32 devices in a mesh: dp: 2 (over x), ctx: 16 (over z, y, core).
Axes of the slice: x: 2, y: 2, z: 4, core: 2. Of those that a mesh axis runs over, the one named last changes fastest.
Arguments:
- queries: bfloat16 [2, 8192, 1024], P('dp', 'ctx'), may hold values from -100 to 100
- key_states: bfloat16 [2, 8192, 128], P('dp', 'ctx'), may hold values from -4 to 4
- value_states: bfloat16 [2, 8192, 128], P('dp', 'ctx'), may hold values from -6 to 6
- doc_ids: int32 [2, 8192], P('dp', 'ctx'), may hold values from 0 to 7, never falling along the last dimension, each value on 1 to 3584 neighbouring positions
Outputs:
- attended: bfloat16 [2, 8192, 1024], P('dp', 'ctx')
The draws below stay inside these ranges and needn't reach their ends.
Inputs may be any that keep to these rules, and one draw needn't show every extreme that they name: `doc_ids`: ids never fall along a sequence; each document spans 1 to 3584 tokens, and one document of each sequence spans exactly 3584.
All inputs are finite; a program needn't handle non-finite values.
Results may differ from the reference program's by a relative error of at most 0.0037.
Values may be sent and summed in bfloat16 or wider, within the bound.
No kernel may reach another device: no remote copies, remote signals or barrier semaphores. Data moves between devices by JAX's collectives and lax.ppermute only.
A program may use at most 64 MiB of HBM per device.

```python
import math
import jax
import jax.numpy as jnp
import numpy as np
from jax import lax

HD = 128
QH = 8
TOK_DEV = 512
SPAN = 7
MICRO = 2
SEQ = 8192
DOC_MAX = 3584
DOCS = 8
N_CTX = 16


def shared_draw(key):
    base = jax.random.fold_in(key, 7)
    key_seed, query_seed = jax.random.split(base, 2)
    keys_raw = jnp.clip(jax.random.normal(key_seed, (MICRO, SEQ, HD), jnp.float32), -4.0, 4.0)
    queries_raw = jnp.clip(jax.random.normal(query_seed, (MICRO, SEQ, QH * HD), jnp.float32), -4.0, 4.0)
    return (queries_raw, keys_raw)


def draw_queries(key, part):
    return shared_draw(key)[0].astype(jnp.bfloat16)


def draw_key_states(key, part):
    return shared_draw(key)[1].astype(jnp.bfloat16)


def level_of(rng, shape, pieces, low, top_value):
    level = 1.0
    for dim, parts in pieces:
        steps = jax.random.uniform(jax.random.fold_in(jax.random.fold_in(rng, 6), dim), (parts,), jnp.float32, low / len(pieces), top_value / len(pieces))
        level = level * jnp.repeat(jnp.exp(steps), shape[dim] // parts).reshape((-1,) + (1,) * (len(shape) - 1 - dim))
    return level


def profile(amount, total, limit, skew):
    loads = [(1 << 20) // math.isqrt(standing ** skew) + 1 for standing in range(2, amount + 1)]
    rest, holding = total - limit - (amount - 1), [1] * (amount - 1)
    while rest > 0:
        candidates = [i for i in range(amount - 1) if holding[i] < limit]
        whole, remaining = sum([loads[i] for i in candidates]), rest
        for i in candidates:
            addition = min(limit - holding[i], max(1, remaining * loads[i] // whole), rest)
            holding[i] = holding[i] + addition
            rest = rest - addition
    return np.array([limit] + holding)


def ragged(stream_key, count, total, bound, lean):
    if count == 2:
        one = jax.random.randint(stream_key, (), max(1, total - bound), min(bound, total - 1) + 1)
        return jnp.stack([one, total - one])
    lengths = jnp.asarray(profile(count, total, bound, lean), jnp.int32)
    pairs = (count - 1) // 2
    giver, receiver = lengths[1:1 + 2 * pairs:2], lengths[2:2 + 2 * pairs:2]
    margin = jnp.minimum(giver - 1, bound - receiver)
    moved = jax.random.randint(jax.random.fold_in(stream_key, 1), (pairs,), 0, 1 << 20) % (margin + 1)
    lengths = lengths.at[1:1 + 2 * pairs:2].set(giver - moved).at[2:2 + 2 * pairs:2].set(receiver + moved)
    return lengths[jax.random.permutation(jax.random.fold_in(stream_key, 2), count)]


def noise(key, extent, deviation, limit, cuts=(), held_as=jnp.bfloat16):
    level = level_of(key, extent, cuts, -0.22, 0.18) if cuts else 1.0
    values = jax.random.normal(key, extent, jnp.float32) * deviation * level
    return jnp.minimum(jnp.maximum(values, -limit), limit).astype(held_as)


def setup_inputs(seed: int = 0) -> dict:
    arg_keys = jax.random.split(jax.random.key(seed), 5)
    return {
        "queries": draw_queries(jax.random.fold_in(arg_keys[4], 71), 0),
        "key_states": draw_key_states(jax.random.fold_in(arg_keys[4], 71), 0),
        "value_states": noise(arg_keys[2], (MICRO, SEQ, HD), 1.0, 6.0, ((0, 2), (1, 16))),
        "doc_ids": jax.vmap(lambda own: jnp.searchsorted(jnp.cumsum(ragged(own, DOCS, SEQ, DOC_MAX, 2)), jnp.arange(SEQ), side="right"))(jax.random.split(arg_keys[3], MICRO)).reshape((MICRO, SEQ)).astype(jnp.int32),
    }


big_negative = -1.0e30


def tile_mask(query_docs, query_pos, key_docs, key_pos):
    return (query_docs[:, None] == key_docs[None, :]) & (key_pos[None, :] <= query_pos[:, None]) & (key_pos[None, :] >= 0)


def empty_state(row_count, head_count, head_size):
    return (jnp.full((row_count, head_count), big_negative, jnp.float32),
            jnp.zeros((row_count, head_count), jnp.float32),
            jnp.zeros((row_count, head_count, head_size), jnp.float32))


def attend_tile(running, query_rows, allowed, key_tile, value_tile, active):
    row_count = allowed.shape[0]
    head_size = query_rows.shape[1]
    head_count = query_rows.shape[0] // row_count

    def compute(previous):
        row_max, row_total, row_accum = previous
        scores = lax.dot_general(query_rows, key_tile, (((1,), (1,)), ((), ())), preferred_element_type=jnp.float32)
        scores = scores.reshape(row_count, head_count, -1) * (head_size ** -0.5)
        visible = allowed[:, None, :]
        masked = jnp.where(visible, scores, big_negative)
        new_max = jnp.maximum(row_max, jnp.max(masked, axis=2))
        weights = jnp.where(visible, jnp.exp(masked - new_max[:, :, None]), 0.0)
        factor = jnp.exp(row_max - new_max)
        row_total = row_total * factor + jnp.sum(weights, axis=2)
        mixed_values = jnp.dot(weights.astype(jnp.bfloat16).reshape(row_count * head_count, -1), value_tile, preferred_element_type=jnp.float32)
        row_accum = row_accum * factor[:, :, None] + mixed_values.reshape(row_count, head_count, head_size)
        return new_max, row_total, row_accum

    return lax.cond(active, compute, lambda previous: previous, running)


def reference(queries, key_states, value_states, doc_ids):
    pad_rows = SPAN * TOK_DEV
    padded_keys = jnp.concatenate([jnp.zeros((MICRO, pad_rows, HD), key_states.dtype), key_states], axis=1)
    padded_values = jnp.concatenate([jnp.zeros((MICRO, pad_rows, HD), value_states.dtype), value_states], axis=1)
    padded_docs = jnp.concatenate([jnp.full((MICRO, pad_rows), -1, jnp.int32), doc_ids.astype(jnp.int32)], axis=1)
    local_pos = jnp.arange(TOK_DEV, dtype=jnp.int32)
    zero_index = jnp.array(0, jnp.int32)

    def one_block(index):
        micro_index = (index // N_CTX).astype(jnp.int32)
        shard_index = (index % N_CTX).astype(jnp.int32)
        row_start = (shard_index * TOK_DEV).astype(jnp.int32)
        query_block = lax.dynamic_slice(queries, (micro_index, row_start, zero_index), (1, TOK_DEV, QH * HD))[0]
        query_rows = query_block.reshape(TOK_DEV * QH, HD)
        query_docs = lax.dynamic_slice(padded_docs, (micro_index, (row_start + pad_rows).astype(jnp.int32)), (1, TOK_DEV))[0]
        query_pos = row_start + local_pos
        running = empty_state(TOK_DEV, QH, HD)
        for offset in range(SPAN + 1):
            start = ((shard_index + SPAN - offset) * TOK_DEV).astype(jnp.int32)
            key_tile = lax.dynamic_slice(padded_keys, (micro_index, start, zero_index), (1, TOK_DEV, HD))[0]
            value_tile = lax.dynamic_slice(padded_values, (micro_index, start, zero_index), (1, TOK_DEV, HD))[0]
            key_docs = lax.dynamic_slice(padded_docs, (micro_index, start), (1, TOK_DEV))[0]
            key_pos = (shard_index - offset) * TOK_DEV + local_pos
            allowed = tile_mask(query_docs, query_pos, key_docs, key_pos)
            running = attend_tile(running, query_rows, allowed, key_tile, value_tile, jnp.any(allowed))
        row_max, row_total, row_accum = running
        return (row_accum / row_total[:, :, None]).astype(jnp.bfloat16)

    blocks = lax.map(one_block, jnp.arange(MICRO * N_CTX, dtype=jnp.int32))
    return blocks.reshape(MICRO, N_CTX * TOK_DEV, QH * HD)
```

```python
import functools
import math

import jax
import jax.numpy as jnp
from jax import lax
from jax.experimental import pallas as pl
from jax.experimental.pallas import tpu as pltpu
from jax.sharding import PartitionSpec as P

SPAN = 7

ROWS = 256
META = 16
NEG = -1e30
KEYS = 256
OWN_GROUP = 2
KEY_LIMIT = 4.0
CALM = 100.0
VMEM_LIMIT = 24 << 20


def pack_kernel(k_ref, v_ref, docs_ref, out_ref):
    tokens, size = k_ref.shape
    out_ref[:tokens, :size] = k_ref[...]
    for start in range(0, tokens, size):
        block = v_ref[start : start + size, :].astype(jnp.float32)
        out_ref[start : start + size, size:] = block.T.astype(jnp.bfloat16)
    width = 2 * size
    ids = (docs_ref[...] + 1).astype(jnp.float32)
    lines = [ids[:, i : i + width] for i in range(0, tokens, width)]
    lines.append(jnp.zeros((META - len(lines), width), jnp.float32))
    out_ref[tokens:, :] = jnp.concatenate(lines, axis=0).astype(jnp.bfloat16)


def pack(k, v, docs):
    tokens, size = k.shape
    return pl.pallas_call(
        pack_kernel,
        out_shape=jax.ShapeDtypeStruct((tokens + META, 2 * size), jnp.bfloat16),
        name="pack",
    )(k, v, docs)


def keys_twice(kv, start, count, size):
    k = kv[start : start + count, :size]
    return jnp.concatenate([k, k], axis=1)


def values_across(kv, start, count, size):
    blocks = [kv[i : i + size, size : 2 * size] for i in range(start, start + count, size)]
    return jnp.concatenate(blocks, axis=1)


def scores_of(keys, q):
    return lax.dot_general(
        keys, q, (((1,), (0,)), ((), ())), preferred_element_type=jnp.float32
    )


def folded(x, op):
    count, width = x.shape
    return op(x.reshape(count // 8, 8, width), axis=0)


def weigh(s, m, l_ref, acc_ref, at, values):
    count, width = s.shape
    p = jnp.exp2(s.reshape(count // 8, 8, width) - m)
    l_ref[at] += jnp.sum(p, axis=0)
    acc_ref[at] += jnp.dot(
        values, p.reshape(count, width).astype(jnp.bfloat16), preferred_element_type=jnp.float32
    )


def weigh_anew(s, m_ref, l_ref, acc_ref, at, values):
    count, width = s.shape
    old = m_ref[at]
    top = jnp.max(jnp.maximum(folded(s, jnp.max), old), axis=0, keepdims=True)
    fade = jnp.exp2(old - top)
    m_ref[at] = jnp.broadcast_to(top, old.shape)
    l_ref[at] *= fade
    acc_ref[at] *= fade[:1]
    weigh(s, m_ref[at], l_ref, acc_ref, at, values)


def pipelined(units):
    ahead = units[0][0]()
    for i, (_, rest) in enumerate(units):
        s = ahead
        if i + 1 < len(units):
            ahead = units[i + 1][0]()
        rest(s)


def own_kernel(q_ref, own_ref, docs_ref, qt_ref, m_ref, l_ref, acc_ref, calm_ref, bias_ref, kt_ref):
    tokens = q_ref.shape[0]
    heads, size = acc_ref.shape[0], acc_ref.shape[1]
    scale = size**-0.5 * math.log2(math.e)
    ids = docs_ref[...].astype(jnp.float32)
    ids_down = jnp.broadcast_to(ids, (size, tokens)).T
    ids_down = jnp.concatenate([ids_down] * (ROWS // size), axis=1)
    for row in range(0, tokens, ROWS):
        count = row + ROWS
        key = lax.broadcasted_iota(jnp.int32, (count, ROWS), 0)
        query = lax.broadcasted_iota(jnp.int32, (count, ROWS), 1) + row
        allowed = (ids_down[:count] == ids[:, row : row + ROWS]) & (key <= query)
        bias_ref[:count, row : row + ROWS] = jnp.where(allowed, 0.0, NEG)
    kt_ref[...] = own_ref[:tokens, :size].astype(jnp.float32).T

    def prepare(h, gap):
        col = pl.multiple_of(h * size, size)
        scaled = (q_ref[:, pl.ds(col, size)].astype(jnp.float32) * scale).T
        high = scaled.astype(jnp.bfloat16)
        low = (scaled - high.astype(jnp.float32)).astype(jnp.bfloat16)
        qt_ref[h, :size, :] = high
        qt_ref[h, size:, :] = low
        own = jnp.sum(scaled * kt_ref[...], axis=0, keepdims=True)
        most = KEY_LIMIT * jnp.sum(jnp.abs(scaled), axis=0, keepdims=True)
        m_ref[h] = jnp.broadcast_to(own, (8, tokens))
        return jnp.maximum(gap, most - own)

    gap = lax.fori_loop(0, heads, prepare, jnp.zeros((1, tokens), jnp.float32))
    calm = jnp.max(gap) <= CALM
    calm_ref[0, 0] = calm.astype(jnp.int32)
    l_ref[...] = jnp.zeros_like(l_ref)
    acc_ref[...] = jnp.zeros_like(acc_ref)

    def units(h):
        made = []
        for row in range(0, tokens, ROWS):
            count = row + ROWS
            cols = slice(row, row + ROWS)

            def scores(count=count, cols=cols):
                s = scores_of(keys_twice(own_ref, 0, count, size), qt_ref[h, :, cols])
                return s + bias_ref[:count, cols]

            def rest(s, count=count, cols=cols):
                at, values = (h, slice(None), cols), values_across(own_ref, 0, count, size)
                weigh(s, m_ref[at], l_ref, acc_ref, at, values)

            def rest_anew(s, count=count, cols=cols):
                at, values = (h, slice(None), cols), values_across(own_ref, 0, count, size)
                weigh_anew(s, m_ref, l_ref, acc_ref, at, values)

            made.append((scores, rest, rest_anew))
        return made

    @pl.when(calm)
    def _():
        def body(i, carry):
            group = [u for g in range(OWN_GROUP) for u in units(OWN_GROUP * i + g)]
            pipelined([(scores, rest) for scores, rest, _ in group])
            return carry

        lax.fori_loop(0, heads // OWN_GROUP, body, 0)

    @pl.when(jnp.logical_not(calm))
    def _():
        def body(h, carry):
            pipelined([(scores, rest) for scores, _, rest in units(h)])
            return carry

        lax.fori_loop(0, heads, body, 0)


def own_part(q, own, docs, heads, size):
    tokens = q.shape[0]
    vmem = pl.BlockSpec(memory_space=pltpu.VMEM)
    return pl.pallas_call(
        own_kernel,
        out_shape=(
            jax.ShapeDtypeStruct((heads, 2 * size, tokens), jnp.bfloat16),
            jax.ShapeDtypeStruct((heads, 8, tokens), jnp.float32),
            jax.ShapeDtypeStruct((heads, 8, tokens), jnp.float32),
            jax.ShapeDtypeStruct((heads, size, tokens), jnp.float32),
            jax.ShapeDtypeStruct((1, 1), jnp.int32),
        ),
        out_specs=(vmem, vmem, vmem, vmem, pl.BlockSpec(memory_space=pltpu.SMEM)),
        scratch_shapes=[
            pltpu.VMEM((tokens, tokens), jnp.float32),
            pltpu.VMEM((size, tokens), jnp.float32),
        ],
        compiler_params=pltpu.CompilerParams(vmem_limit_bytes=VMEM_LIMIT),
        name="own_part",
    )(q, own, docs)


def earlier_kernel(count, last, *refs):
    calm_ref, qt_ref, docs_ref = refs[:3]
    sources = refs[3 : 3 + count]
    m_in, l_in, acc_in = refs[3 + count : 6 + count]
    rest = refs[6 + count :]
    if last:
        out_ref, m_ref, l_ref, acc_ref = rest[0], m_in, l_in, acc_in
        rest = rest[1:]
    else:
        m_ref, l_ref, acc_ref = rest[:3]
        rest = rest[3:]
    kv_ref, bias_ref, sems = rest
    heads, size, tokens = acc_in.shape
    calm = calm_ref[0, 0] == 1

    def copy(j):
        return pltpu.make_async_copy(sources[j], kv_ref.at[j], sems.at[j])

    for j in range(count):
        copy(j).start()
    ids = docs_ref[...].astype(jnp.float32)
    first = jnp.min(ids)
    rows = jnp.sum(jnp.where(ids == first, 1.0, 0.0)).astype(jnp.int32)
    for j in range(count):
        copy(j).wait()

    def unit(kv, h, row, start, keys, bias=None, anew=False):
        at = (h, slice(None), pl.ds(row, ROWS))

        def scores():
            s = scores_of(keys_twice(kv, start, keys, size), qt_ref[at])
            return s if bias is None else s + bias[start : start + keys, :]

        def rest(s):
            values = values_across(kv, start, keys, size)
            if anew:
                weigh_anew(s, m_ref, l_ref, acc_ref, at, values)
            else:
                weigh(s, m_ref[at], l_ref, acc_ref, at, values)

        return scores, rest

    def shard(j, carry):
        kv = kv_ref.at[j]
        marks = kv[tokens:, :].astype(jnp.float32)
        valid = jnp.sum(jnp.where(marks == first + 1.0, 1.0, 0.0)).astype(jnp.int32)
        whole = (valid == tokens) & (rows == tokens) & calm

        @pl.when(whole)
        def _():
            pipelined([
                unit(kv, h, row, start, KEYS)
                for h in range(heads)
                for row in range(0, tokens, ROWS)
                for start in range(0, tokens, KEYS)
            ])

        def partly(anew, group):
            def block(i, carry):
                row = pl.multiple_of(i * ROWS, ROWS)
                key = lax.broadcasted_iota(jnp.int32, (tokens, ROWS), 0)
                query = lax.broadcasted_iota(jnp.int32, (tokens, ROWS), 1) + row
                allowed = (key >= tokens - valid) & (query < rows)
                bias_ref[...] = jnp.where(allowed, 0.0, NEG)
                for start in range(0, tokens, ROWS):
                    @pl.when(valid > tokens - start - ROWS)
                    def _():
                        def some(g, carry):
                            pipelined([
                                unit(kv, group * g + h, row, start, ROWS, bias_ref, anew)
                                for h in range(group)
                            ])
                            return carry

                        lax.fori_loop(0, heads // group, some, 0)
                return carry

            lax.fori_loop(0, (rows + ROWS - 1) // ROWS, block, 0)

        @pl.when((valid > 0) & calm & jnp.logical_not(whole))
        def _():
            partly(False, 4)

        @pl.when((valid > 0) & jnp.logical_not(calm))
        def _():
            partly(True, 1)

        return carry

    lax.fori_loop(0, count, shard, 0)

    if last:
        for h in range(heads):
            total = jnp.sum(l_ref[h], axis=0, keepdims=True)
            done = acc_ref[h] * (1.0 / total)
            out_ref[:, h * size : (h + 1) * size] = done.T.astype(jnp.bfloat16)


def earlier_part(calm, qt, docs, shards, state, last):
    heads, double, tokens = qt.shape
    size = double // 2
    count = len(shards)
    vmem = pl.BlockSpec(memory_space=pltpu.VMEM)
    if last:
        out_shape = jax.ShapeDtypeStruct((tokens, heads * size), jnp.bfloat16)
        aliases = {}
    else:
        out_shape = tuple(jax.ShapeDtypeStruct(s.shape, s.dtype) for s in state)
        aliases = {3 + count + i: i for i in range(3)}
    return pl.pallas_call(
        functools.partial(earlier_kernel, count, last),
        out_shape=out_shape,
        in_specs=[pl.BlockSpec(memory_space=pltpu.SMEM), vmem, vmem]
        + [pl.BlockSpec(memory_space=pltpu.HBM)] * count
        + [vmem] * 3,
        scratch_shapes=[
            pltpu.VMEM((count,) + shards[0].shape, jnp.bfloat16),
            pltpu.VMEM((tokens, ROWS), jnp.float32),
            pltpu.SemaphoreType.DMA((count,)),
        ],
        input_output_aliases=aliases,
        compiler_params=pltpu.CompilerParams(vmem_limit_bytes=VMEM_LIMIT),
        name="earlier_part_last" if last else "earlier_part",
    )(calm, qt, docs, *shards, *state)


def send(x, by, who=(0, 1, 2, 3)):
    length = lax.axis_size("ctx")
    pairs = [(i, i + by) for i in range(length) if i % 4 in who]
    return lax.ppermute(x, "ctx", [(i, j) for i, j in pairs if 0 <= j < length])


def swap(x, mask, who=(0, 1, 2, 3)):
    length = lax.axis_size("ctx")
    return lax.ppermute(x, "ctx", [(i, i ^ mask) for i in range(length) if i % 4 in who])


def on_device(queries, key_states, value_states, doc_ids):
    size = key_states.shape[2]
    heads = queries.shape[2] // size
    own = pack(key_states[0], value_states[0], doc_ids)
    before = send(own, 4)
    near = send(own, 2, (0, 1))
    beside = send(own, 1, (0, 2))
    qt, *state, calm = own_part(queries[0], own, doc_ids, heads, size)
    across = swap(before, 2)
    beside_before = swap(before, 1)
    far = send(before, 2, (2, 3))
    farthest = send(before, 3, (1, 3))
    beside_near = swap(near, 1, (2, 3))
    beside_across = swap(across, 1)
    beside_far = swap(far, 1, (0, 1))
    early = [beside, before, beside_before, near, beside_near]
    state = earlier_part(calm, qt, doc_ids, early, state, False)
    late = [across, beside_across]
    state = earlier_part(calm, qt, doc_ids, late, state, False)
    last = [far, beside_far, farthest]
    out = earlier_part(calm, qt, doc_ids, last, state, True)
    return out[None]


def solution(mesh):
    in_specs = (P("dp", "ctx", None), P("dp", "ctx", None), P("dp", "ctx", None), P("dp", "ctx"))
    out_specs = P("dp", "ctx", None)
    return jax.shard_map(
        on_device, mesh=mesh, in_specs=in_specs, out_specs=out_specs, check_vma=False
    )
```

```python
import functools
import math

import jax
import jax.numpy as jnp
from jax import lax
from jax.experimental import pallas as pl
from jax.experimental.pallas import tpu as pltpu
from jax.sharding import PartitionSpec as P

SPAN = 7

ROWS = 256
META = 16
NEG = -1e30
KEYS = 256
AHEAD = 6
FLAGS = {}
OWN_GROUP = 8
KEY_LIMIT = 4.0
CALM = 100.0
VMEM_LIMIT = 24 << 20


def pack_kernel(k_ref, v_ref, docs_ref, out_ref):
    tokens, size = k_ref.shape
    out_ref[:tokens, :size] = k_ref[...]
    for start in range(0, tokens, size):
        block = v_ref[start : start + size, :].astype(jnp.float32)
        out_ref[start : start + size, size:] = block.T.astype(jnp.bfloat16)
    width = 2 * size
    ids = (docs_ref[...] + 1).astype(jnp.float32)
    lines = [ids[:, i : i + width] for i in range(0, tokens, width)]
    lines.append(jnp.zeros((META - len(lines), width), jnp.float32))
    out_ref[tokens:, :] = jnp.concatenate(lines, axis=0).astype(jnp.bfloat16)


def pack(k, v, docs):
    tokens, size = k.shape
    return pl.pallas_call(
        pack_kernel,
        out_shape=jax.ShapeDtypeStruct((tokens + META, 2 * size), jnp.bfloat16),
        name="pack",
    )(k, v, docs)


def keys_twice(kv, start, count, size):
    k = kv[start : start + count, :size]
    return jnp.concatenate([k, k], axis=1)


def values_across(kv, start, count, size):
    blocks = [kv[i : i + size, size : 2 * size] for i in range(start, start + count, size)]
    return jnp.concatenate(blocks, axis=1)


def scores_of(keys, q):
    return lax.dot_general(
        keys, q, (((1,), (0,)), ((), ())), preferred_element_type=jnp.float32
    )


def folded(x, op):
    count, width = x.shape
    return op(x.reshape(count // 8, 8, width), axis=0)


def weigh(s, m, l_ref, acc_ref, at, values):
    count, width = s.shape
    p = jnp.exp2(s.reshape(count // 8, 8, width) - m)
    l_ref[at] += jnp.sum(p, axis=0)
    acc_ref[at] += jnp.dot(
        values, p.reshape(count, width).astype(jnp.bfloat16), preferred_element_type=jnp.float32
    )


def weigh_anew(s, m_ref, l_ref, acc_ref, at, values):
    count, width = s.shape
    old = m_ref[at]
    top = jnp.max(jnp.maximum(folded(s, jnp.max), old), axis=0, keepdims=True)
    fade = jnp.exp2(old - top)
    m_ref[at] = jnp.broadcast_to(top, old.shape)
    l_ref[at] *= fade
    acc_ref[at] *= fade[:1]
    weigh(s, m_ref[at], l_ref, acc_ref, at, values)


def pipelined(units):
    ahead = [scores() for scores, _ in units[:AHEAD]]
    for i, (_, rest) in enumerate(units):
        if i + AHEAD < len(units):
            ahead.append(units[i + AHEAD][0]())
        rest(ahead.pop(0))


def own_kernel(
    q_hbm, own_hbm, docs_hbm, qt_ref, m_ref, l_ref, acc_ref, facts_ref,
    q_ref, own_ref, docs_ref, bias_ref, kt_ref, sems,
):
    copies = [
        pltpu.make_async_copy(docs_hbm, docs_ref, sems.at[0]),
        pltpu.make_async_copy(own_hbm, own_ref, sems.at[1]),
        pltpu.make_async_copy(q_hbm, q_ref, sems.at[2]),
    ]
    for copy in copies:
        copy.start()
    tokens = q_ref.shape[0]
    heads, size = acc_ref.shape[0], acc_ref.shape[1]
    scale = size**-0.5 * math.log2(math.e)
    copies[0].wait()
    ids = docs_ref[...].astype(jnp.float32)
    ids_down = jnp.broadcast_to(ids, (size, tokens)).T
    ids_down = jnp.concatenate([ids_down] * (ROWS // size), axis=1)
    for row in range(0, tokens, ROWS):
        count = row + ROWS
        key = lax.broadcasted_iota(jnp.int32, (count, ROWS), 0)
        query = lax.broadcasted_iota(jnp.int32, (count, ROWS), 1) + row
        allowed = (ids_down[:count] == ids[:, row : row + ROWS]) & (key <= query)
        bias_ref[:count, row : row + ROWS] = jnp.where(allowed, 0.0, NEG)
    first = jnp.min(ids)
    facts_ref[0, 1] = first.astype(jnp.int32) + 1
    facts_ref[0, 2] = jnp.sum(jnp.where(ids == first, 1.0, 0.0)).astype(jnp.int32)
    l_ref[...] = jnp.zeros_like(l_ref)
    acc_ref[...] = jnp.zeros_like(acc_ref)
    copies[1].wait()
    kt_ref[...] = own_ref[:tokens, :size].T.astype(jnp.float32)
    copies[2].wait()

    def prepare(h, gap):
        col = pl.multiple_of(h * size, size)
        scaled = q_ref[:, pl.ds(col, size)].T.astype(jnp.float32) * scale
        high = scaled.astype(jnp.bfloat16)
        low = (scaled - high.astype(jnp.float32)).astype(jnp.bfloat16)
        qt_ref[h, :size, :] = high
        qt_ref[h, size:, :] = low
        own = jnp.sum(scaled * kt_ref[...], axis=0, keepdims=True)
        most = KEY_LIMIT * jnp.sum(jnp.abs(scaled), axis=0, keepdims=True)
        m_ref[h] = jnp.broadcast_to(own, (8, tokens))
        return jnp.maximum(gap, most - own)

    gap = jnp.zeros((1, tokens), jnp.float32)
    for h in range(heads):
        gap = prepare(h, gap)
    calm = jnp.max(gap) <= CALM
    facts_ref[0, 0] = calm.astype(jnp.int32)

    def units(h):
        made = []
        for row in range(0, tokens, ROWS):
            count = row + ROWS
            cols = slice(row, row + ROWS)

            def scores(count=count, cols=cols):
                s = scores_of(keys_twice(own_ref, 0, count, size), qt_ref[h, :, cols])
                return s + bias_ref[:count, cols]

            def rest(s, count=count, cols=cols):
                at, values = (h, slice(None), cols), values_across(own_ref, 0, count, size)
                weigh(s, m_ref[at], l_ref, acc_ref, at, values)

            def rest_anew(s, count=count, cols=cols):
                at, values = (h, slice(None), cols), values_across(own_ref, 0, count, size)
                weigh_anew(s, m_ref, l_ref, acc_ref, at, values)

            made.append((scores, rest, rest_anew))
        return made

    @pl.when(calm)
    def _():
        def body(i, carry):
            group = [u for g in range(OWN_GROUP) for u in units(OWN_GROUP * i + g)]
            pipelined([(scores, rest) for scores, rest, _ in group])
            return carry

        lax.fori_loop(0, heads // OWN_GROUP, body, 0)

    @pl.when(jnp.logical_not(calm))
    def _():
        def body(h, carry):
            pipelined([(scores, rest) for scores, _, rest in units(h)])
            return carry

        lax.fori_loop(0, heads, body, 0)


def own_part(q, own, docs, heads, size):
    tokens = q.shape[0]
    vmem = pl.BlockSpec(memory_space=pltpu.VMEM)
    q, own, docs = (pltpu.with_memory_space_constraint(x, pltpu.HBM) for x in (q, own, docs))
    return pl.pallas_call(
        own_kernel,
        out_shape=(
            jax.ShapeDtypeStruct((heads, 2 * size, tokens), jnp.bfloat16),
            jax.ShapeDtypeStruct((heads, 8, tokens), jnp.float32),
            jax.ShapeDtypeStruct((heads, 8, tokens), jnp.float32),
            jax.ShapeDtypeStruct((heads, size, tokens), jnp.float32),
            jax.ShapeDtypeStruct((1, 3), jnp.int32),
        ),
        in_specs=[pl.BlockSpec(memory_space=pltpu.HBM)] * 3,
        out_specs=(vmem, vmem, vmem, vmem, pl.BlockSpec(memory_space=pltpu.SMEM)),
        scratch_shapes=[
            pltpu.VMEM(q.shape, q.dtype),
            pltpu.VMEM(own.shape, own.dtype),
            pltpu.VMEM(docs.shape, docs.dtype),
            pltpu.VMEM((tokens, tokens), jnp.float32),
            pltpu.VMEM((size, tokens), jnp.float32),
            pltpu.SemaphoreType.DMA((3,)),
        ],
        compiler_params=pltpu.CompilerParams(vmem_limit_bytes=VMEM_LIMIT, flags=FLAGS),
        name="own_part",
    )(q, own, docs)


def earlier_kernel(count, last, *refs):
    facts_ref, qt_ref = refs[:2]
    sources = refs[2 : 2 + count]
    m_in, l_in, acc_in = refs[2 + count : 5 + count]
    rest = refs[5 + count :]
    if last:
        out_hbm, m_ref, l_ref, acc_ref = rest[0], m_in, l_in, acc_in
        out_ref, out_sems = rest[-2:]
        rest = rest[1:-2]
    else:
        m_ref, l_ref, acc_ref = rest[:3]
        rest = rest[3:]
    kv_ref, bias_ref, valid_ref, sems = rest
    heads, size, tokens = acc_in.shape
    calm = facts_ref[0, 0] == 1
    first = facts_ref[0, 1].astype(jnp.float32)
    rows = facts_ref[0, 2]

    copies = [
        pltpu.make_async_copy(sources[j], kv_ref.at[j], sems.at[j]) for j in range(count)
    ]
    for copy in copies:
        copy.start()
    for copy in copies:
        copy.wait()
    found = [
        jnp.sum(jnp.where(kv_ref[j, tokens:, :].astype(jnp.float32) == first, 1.0, 0.0))
        for j in range(count)
    ]
    for j in range(count):
        valid_ref[j] = found[j].astype(jnp.int32)

    def unit(kv, h, row, start, keys, bias=None, anew=False):
        at = (h, slice(None), pl.ds(row, ROWS))

        def scores():
            s = scores_of(keys_twice(kv, start, keys, size), qt_ref[at])
            return s if bias is None else s + bias[start : start + keys, :]

        def rest(s):
            values = values_across(kv, start, keys, size)
            if anew:
                weigh_anew(s, m_ref, l_ref, acc_ref, at, values)
            else:
                weigh(s, m_ref[at], l_ref, acc_ref, at, values)

        return scores, rest

    def shard(j, carry):
        kv = kv_ref.at[j]
        valid = valid_ref[j]
        whole = (valid == tokens) & (rows == tokens) & calm

        @pl.when(whole)
        def _():
            pipelined([
                unit(kv, h, row, start, KEYS)
                for h in range(heads)
                for row in range(0, tokens, ROWS)
                for start in range(0, tokens, KEYS)
            ])

        def partly(anew, group):
            def block(i, carry):
                row = pl.multiple_of(i * ROWS, ROWS)
                key = lax.broadcasted_iota(jnp.int32, (tokens, ROWS), 0)
                query = lax.broadcasted_iota(jnp.int32, (tokens, ROWS), 1) + row
                allowed = (key >= tokens - valid) & (query < rows)
                bias_ref[...] = jnp.where(allowed, 0.0, NEG)
                for start in range(0, tokens, ROWS):
                    @pl.when(valid > tokens - start - ROWS)
                    def _():
                        def some(g, carry):
                            pipelined([
                                unit(kv, group * g + h, row, start, ROWS, bias_ref, anew)
                                for h in range(group)
                            ])
                            return carry

                        lax.fori_loop(0, heads // group, some, 0)
                return carry

            lax.fori_loop(0, (rows + ROWS - 1) // ROWS, block, 0)

        @pl.when((valid > 0) & calm & jnp.logical_not(whole))
        def _():
            partly(False, 4)

        @pl.when((valid > 0) & jnp.logical_not(calm))
        def _():
            partly(True, 1)

        return carry

    lax.fori_loop(0, count, shard, 0)

    if last:
        copies = []
        for h in range(heads):
            total = jnp.sum(l_ref[h], axis=0, keepdims=True)
            done = (acc_ref[h] * (1.0 / total)).astype(jnp.bfloat16)
            cols = slice(h * size, (h + 1) * size)
            out_ref[:, cols] = done.T
            copies.append(
                pltpu.make_async_copy(out_ref.at[:, cols], out_hbm.at[:, cols], out_sems.at[h])
            )
            copies[-1].start()
        for copy in copies:
            copy.wait()


def earlier_part(facts, qt, shards, state, last):
    heads, double, tokens = qt.shape
    size = double // 2
    count = len(shards)
    vmem = pl.BlockSpec(memory_space=pltpu.VMEM)
    hbm = pl.BlockSpec(memory_space=pltpu.HBM)
    scratch = [
        pltpu.VMEM((count,) + shards[0].shape, jnp.bfloat16),
        pltpu.VMEM((tokens, ROWS), jnp.float32),
        pltpu.SMEM((count,), jnp.int32),
        pltpu.SemaphoreType.DMA((count,)),
    ]
    if last:
        out_shape = jax.ShapeDtypeStruct((tokens, heads * size), jnp.bfloat16)
        out_specs = hbm
        aliases = {}
        scratch += [pltpu.VMEM(out_shape.shape, jnp.bfloat16), pltpu.SemaphoreType.DMA((heads,))]
    else:
        out_shape = tuple(jax.ShapeDtypeStruct(s.shape, s.dtype) for s in state)
        out_specs = (vmem,) * 3
        aliases = {2 + count + i: i for i in range(3)}
    return pl.pallas_call(
        functools.partial(earlier_kernel, count, last),
        out_shape=out_shape,
        in_specs=[pl.BlockSpec(memory_space=pltpu.SMEM), vmem] + [hbm] * count + [vmem] * 3,
        out_specs=out_specs,
        scratch_shapes=scratch,
        input_output_aliases=aliases,
        compiler_params=pltpu.CompilerParams(vmem_limit_bytes=VMEM_LIMIT, flags=FLAGS),
        name="earlier_part_last" if last else "earlier_part",
    )(facts, qt, *shards, *state)


def send(x, by, who=(0, 1, 2, 3)):
    length = lax.axis_size("ctx")
    pairs = [(i, i + by) for i in range(length) if i % 4 in who]
    return lax.ppermute(x, "ctx", [(i, j) for i, j in pairs if 0 <= j < length])


def swap(x, mask, who=(0, 1, 2, 3)):
    length = lax.axis_size("ctx")
    return lax.ppermute(x, "ctx", [(i, i ^ mask) for i in range(length) if i % 4 in who])


def on_device(queries, key_states, value_states, doc_ids):
    size = key_states.shape[2]
    heads = queries.shape[2] // size
    own = pack(key_states[0], value_states[0], doc_ids)
    before = send(own, 4)
    length = lax.axis_size("ctx")
    across = lax.ppermute(own, "ctx", [(i, (i + 4) ^ 2) for i in range(length - 4)])
    near = send(own, 2, (0, 1))
    beside = send(own, 1, (0, 2))
    qt, *state, facts = own_part(queries[0], own, doc_ids, heads, size)
    before, facts = lax.optimization_barrier((before, facts))
    beside_before = swap(before, 1)
    beside_near = swap(near, 1, (2, 3))
    far = send(before, 2, (2, 3))
    farthest = send(before, 3, (1, 3))
    beside_across = swap(across, 1)
    early = [beside, near, before, beside_before, beside_near, across, beside_across]
    state = earlier_part(facts, qt, early, state, False)
    far, state = lax.optimization_barrier((far, state))
    beside_far = swap(far, 1, (0, 1))
    out = earlier_part(facts, qt, [far, farthest, beside_far], state, True)
    return out[None]


def solution(mesh):
    in_specs = (P("dp", "ctx", None), P("dp", "ctx", None), P("dp", "ctx", None), P("dp", "ctx"))
    out_specs = P("dp", "ctx", None)
    return jax.shard_map(
        on_device, mesh=mesh, in_specs=in_specs, out_specs=out_specs, check_vma=False
    )
```

```python
import functools
import math

import jax
import jax.numpy as jnp
from jax import lax
from jax.experimental import pallas as pl
from jax.experimental.pallas import tpu as pltpu
from jax.sharding import PartitionSpec as P


ROWS = 256
META = 16
NEG = -1e30
KEYS = 256
AHEAD = 6
OWN_GROUP = 8
KEY_LIMIT = 4.0
CALM = 100.0
VMEM_LIMIT = 24 << 20


def pack_kernel(k_ref, v_ref, docs_ref, out_ref):
    tokens, size = k_ref.shape
    out_ref[:tokens, :size] = k_ref[...]
    for start in range(0, tokens, size):
        block = v_ref[start : start + size, :].astype(jnp.float32)
        out_ref[start : start + size, size:] = block.T.astype(jnp.bfloat16)
    width = 2 * size
    ids = (docs_ref[...] + 1).astype(jnp.float32)
    lines = [ids[:, i : i + width] for i in range(0, tokens, width)]
    lines.append(jnp.zeros((META - len(lines), width), jnp.float32))
    out_ref[tokens:, :] = jnp.concatenate(lines, axis=0).astype(jnp.bfloat16)


def pack(k, v, docs):
    tokens, size = k.shape
    return pl.pallas_call(
        pack_kernel,
        out_shape=jax.ShapeDtypeStruct((tokens + META, 2 * size), jnp.bfloat16),
        name="pack",
    )(k, v, docs)


def keys_twice(kv, start, count, size):
    k = kv[pl.ds(start, count), :size]
    return jnp.concatenate([k, k], axis=1)


def values_across(kv, start, count, size):
    blocks = [kv[pl.ds(start + i, size), size : 2 * size] for i in range(0, count, size)]
    return jnp.concatenate(blocks, axis=1)


def scores_of(keys, q):
    return lax.dot_general(
        keys, q, (((1,), (0,)), ((), ())), preferred_element_type=jnp.float32
    )


def folded(x, op):
    count, width = x.shape
    return op(x.reshape(count // 8, 8, width), axis=0)


def weigh(s, m, l_ref, acc_ref, at, values):
    count, width = s.shape
    p = jnp.exp2(s.reshape(count // 8, 8, width) - m)
    l_ref[at] += jnp.sum(p, axis=0)
    acc_ref[at] += jnp.dot(
        values, p.reshape(count, width).astype(jnp.bfloat16), preferred_element_type=jnp.float32
    )


def weigh_anew(s, m_ref, l_ref, acc_ref, at, values):
    old = m_ref[at]
    top = jnp.max(jnp.maximum(folded(s, jnp.max), old), axis=0, keepdims=True)
    fade = jnp.exp2(old - top)
    m_ref[at] = jnp.broadcast_to(top, old.shape)
    l_ref[at] *= fade
    acc_ref[at] *= fade[:1]
    weigh(s, m_ref[at], l_ref, acc_ref, at, values)


def pipelined(units):
    ahead = [scores() for scores, _ in units[:AHEAD]]
    for i, (_, rest) in enumerate(units):
        if i + AHEAD < len(units):
            ahead.append(units[i + AHEAD][0]())
        rest(ahead.pop(0))


def own_kernel(
    q_hbm, own_hbm, docs_hbm, qt_ref, m_ref, l_ref, acc_ref, facts_ref,
    q_ref, own_ref, docs_ref, bias_ref, kt_ref, sems,
):
    copies = [
        pltpu.make_async_copy(docs_hbm, docs_ref, sems.at[0]),
        pltpu.make_async_copy(own_hbm, own_ref, sems.at[1]),
        pltpu.make_async_copy(q_hbm, q_ref, sems.at[2]),
    ]
    for copy in copies:
        copy.start()
    tokens = q_ref.shape[0]
    heads, size = acc_ref.shape[0], acc_ref.shape[1]
    scale = size**-0.5 * math.log2(math.e)
    copies[0].wait()
    ids = docs_ref[...].astype(jnp.float32)
    ids_down = jnp.broadcast_to(ids, (size, tokens)).T
    ids_down = jnp.concatenate([ids_down] * (ROWS // size), axis=1)
    for row in range(0, tokens, ROWS):
        count = row + ROWS
        key = lax.broadcasted_iota(jnp.int32, (count, ROWS), 0)
        query = lax.broadcasted_iota(jnp.int32, (count, ROWS), 1) + row
        allowed = (ids_down[:count] == ids[:, row : row + ROWS]) & (key <= query)
        bias_ref[:count, row : row + ROWS] = jnp.where(allowed, 0.0, NEG)
    first = jnp.min(ids)
    facts_ref[0, 1] = first.astype(jnp.int32) + 1
    facts_ref[0, 2] = jnp.sum(jnp.where(ids == first, 1.0, 0.0)).astype(jnp.int32)
    l_ref[...] = jnp.zeros_like(l_ref)
    acc_ref[...] = jnp.zeros_like(acc_ref)
    copies[1].wait()
    kt_ref[...] = own_ref[:tokens, :size].T.astype(jnp.float32)
    copies[2].wait()

    def prepare(h, gap):
        col = pl.multiple_of(h * size, size)
        scaled = q_ref[:, pl.ds(col, size)].T.astype(jnp.float32) * scale
        high = scaled.astype(jnp.bfloat16)
        low = (scaled - high.astype(jnp.float32)).astype(jnp.bfloat16)
        qt_ref[h, :size, :] = high
        qt_ref[h, size:, :] = low
        own = jnp.sum(scaled * kt_ref[...], axis=0, keepdims=True)
        most = KEY_LIMIT * jnp.sum(jnp.abs(scaled), axis=0, keepdims=True)
        m_ref[h] = jnp.broadcast_to(own, (8, tokens))
        return jnp.maximum(gap, most - own)

    gap = jnp.zeros((1, tokens), jnp.float32)
    for h in range(heads):
        gap = prepare(h, gap)
    calm = jnp.max(gap) <= CALM
    facts_ref[0, 0] = calm.astype(jnp.int32)

    def units(h):
        made = []
        for row in range(0, tokens, ROWS):
            count = row + ROWS
            cols = slice(row, row + ROWS)

            def scores(count=count, cols=cols):
                s = scores_of(keys_twice(own_ref, 0, count, size), qt_ref[h, :, cols])
                return s + bias_ref[:count, cols]

            def rest(s, count=count, cols=cols):
                at, values = (h, slice(None), cols), values_across(own_ref, 0, count, size)
                weigh(s, m_ref[at], l_ref, acc_ref, at, values)

            def rest_anew(s, count=count, cols=cols):
                at, values = (h, slice(None), cols), values_across(own_ref, 0, count, size)
                weigh_anew(s, m_ref, l_ref, acc_ref, at, values)

            made.append((scores, rest, rest_anew))
        return made

    @pl.when(calm)
    def _():
        def body(i, carry):
            group = [u for g in range(OWN_GROUP) for u in units(OWN_GROUP * i + g)]
            pipelined([(scores, rest) for scores, rest, _ in group])
            return carry

        lax.fori_loop(0, heads // OWN_GROUP, body, 0)

    @pl.when(jnp.logical_not(calm))
    def _():
        def body(h, carry):
            pipelined([(scores, rest) for scores, _, rest in units(h)])
            return carry

        lax.fori_loop(0, heads, body, 0)


def own_part(q, own, docs, heads, size):
    tokens = q.shape[0]
    vmem = pl.BlockSpec(memory_space=pltpu.VMEM)
    q, own, docs = (pltpu.with_memory_space_constraint(x, pltpu.HBM) for x in (q, own, docs))
    return pl.pallas_call(
        own_kernel,
        out_shape=(
            jax.ShapeDtypeStruct((heads, 2 * size, tokens), jnp.bfloat16),
            jax.ShapeDtypeStruct((heads, 8, tokens), jnp.float32),
            jax.ShapeDtypeStruct((heads, 8, tokens), jnp.float32),
            jax.ShapeDtypeStruct((heads, size, tokens), jnp.float32),
            jax.ShapeDtypeStruct((1, 3), jnp.int32),
        ),
        in_specs=[pl.BlockSpec(memory_space=pltpu.HBM)] * 3,
        out_specs=(vmem, vmem, vmem, vmem, pl.BlockSpec(memory_space=pltpu.SMEM)),
        scratch_shapes=[
            pltpu.VMEM(q.shape, q.dtype),
            pltpu.VMEM(own.shape, own.dtype),
            pltpu.VMEM(docs.shape, docs.dtype),
            pltpu.VMEM((tokens, tokens), jnp.float32),
            pltpu.VMEM((size, tokens), jnp.float32),
            pltpu.SemaphoreType.DMA((3,)),
        ],
        compiler_params=pltpu.CompilerParams(vmem_limit_bytes=VMEM_LIMIT),
        name="own_part",
    )(q, own, docs)


def earlier_kernel(count, last, *refs):
    facts_ref, qt_ref = refs[:2]
    sources = refs[2 : 2 + count]
    m_in, l_in, acc_in = refs[2 + count : 5 + count]
    rest = refs[5 + count :]
    if last:
        out_hbm, m_ref, l_ref, acc_ref = rest[0], m_in, l_in, acc_in
        out_ref, out_sems = rest[-2:]
        rest = rest[1:-2]
    else:
        m_ref, l_ref, acc_ref = rest[:3]
        rest = rest[3:]
    kv_ref, bias_ref, valid_ref, sems = rest
    heads, size, tokens = acc_in.shape
    calm = facts_ref[0, 0] == 1
    first = facts_ref[0, 1].astype(jnp.float32)
    rows = facts_ref[0, 2]

    copies = [
        pltpu.make_async_copy(sources[j], kv_ref.at[j], sems.at[j]) for j in range(count)
    ]
    for copy in copies:
        copy.start()
    for copy in copies:
        copy.wait()
    found = [
        jnp.sum(jnp.where(kv_ref[j, tokens:, :].astype(jnp.float32) == first, 1.0, 0.0))
        for j in range(count)
    ]
    for j in range(count):
        valid_ref[j] = found[j].astype(jnp.int32)

    def unit(kv, h, row, start, keys, bias=None, anew=False):
        at = (h, slice(None), pl.ds(row, ROWS))

        def scores():
            s = scores_of(keys_twice(kv, start, keys, size), qt_ref[at])
            return s if bias is None else s + bias[pl.ds(start, keys), :]

        def rest(s):
            values = values_across(kv, start, keys, size)
            if anew:
                weigh_anew(s, m_ref, l_ref, acc_ref, at, values)
            else:
                query = lax.broadcasted_iota(jnp.int32, (8, ROWS), 1) + row
                m = jnp.where(query < rows, m_ref[at], -NEG)
                weigh(s, m, l_ref, acc_ref, at, values)

        return scores, rest

    def shard(j, carry):
        kv = kv_ref.at[j]
        valid = valid_ref[j]
        whole = calm & (valid == tokens)
        many = rows > tokens - ROWS

        def full(blocks):
            pipelined([
                unit(kv, h, row, start, KEYS)
                for h in range(heads)
                for row in blocks
                for start in range(0, tokens, KEYS)
            ])

        def blocks_of(work):
            def block(i, carry):
                work(pl.multiple_of(i * ROWS, ROWS))
                return carry

            lax.fori_loop(0, (rows + ROWS - 1) // ROWS, block, 0)

        @pl.when(whole & many)
        def _():
            full(range(0, tokens, ROWS))

        @pl.when(whole & jnp.logical_not(many))
        def _():
            blocks_of(lambda row: full([row]))

        def partly(anew, group):
            key = lax.broadcasted_iota(jnp.int32, (tokens, ROWS), 0)
            missing = jnp.where(key >= tokens - valid, 0.0, NEG)

            def work(row):
                query = lax.broadcasted_iota(jnp.int32, (8, ROWS), 1) + row
                if anew:
                    bias_ref[...] = jnp.where((query < rows)[:1], missing, NEG)
                else:
                    bias_ref[...] = missing

                def half(i, carry):
                    start = pl.multiple_of(i * ROWS, ROWS)

                    def some(g, carry):
                        pipelined([
                            unit(kv, group * g + h, row, start, ROWS, bias_ref, anew)
                            for h in range(group)
                        ])
                        return carry

                    if group == heads:
                        some(0, 0)
                    else:
                        lax.fori_loop(0, heads // group, some, 0)
                    return carry

                lax.fori_loop((tokens - valid) // ROWS, tokens // ROWS, half, 0)

            blocks_of(work)

        @pl.when((valid > 0) & calm & jnp.logical_not(whole))
        def _():
            partly(False, heads)

        @pl.when((valid > 0) & jnp.logical_not(calm))
        def _():
            partly(True, 1)

        return carry

    lax.fori_loop(0, count, shard, 0)

    if last:
        copies = []
        for h in range(heads):
            total = jnp.sum(l_ref[h], axis=0, keepdims=True)
            done = (acc_ref[h] * (1.0 / total)).astype(jnp.bfloat16)
            cols = slice(h * size, (h + 1) * size)
            out_ref[:, cols] = done.T
            copies.append(
                pltpu.make_async_copy(out_ref.at[:, cols], out_hbm.at[:, cols], out_sems.at[h])
            )
            copies[-1].start()
        for copy in copies:
            copy.wait()


def earlier_part(facts, qt, shards, state, last):
    heads, double, tokens = qt.shape
    size = double // 2
    count = len(shards)
    vmem = pl.BlockSpec(memory_space=pltpu.VMEM)
    hbm = pl.BlockSpec(memory_space=pltpu.HBM)
    scratch = [
        pltpu.VMEM((count,) + shards[0].shape, jnp.bfloat16),
        pltpu.VMEM((tokens, ROWS), jnp.float32),
        pltpu.SMEM((count,), jnp.int32),
        pltpu.SemaphoreType.DMA((count,)),
    ]
    if last:
        out_shape = jax.ShapeDtypeStruct((tokens, heads * size), jnp.bfloat16)
        out_specs = hbm
        aliases = {}
        scratch += [pltpu.VMEM(out_shape.shape, jnp.bfloat16), pltpu.SemaphoreType.DMA((heads,))]
    else:
        out_shape = tuple(jax.ShapeDtypeStruct(s.shape, s.dtype) for s in state)
        out_specs = (vmem,) * 3
        aliases = {2 + count + i: i for i in range(3)}
    return pl.pallas_call(
        functools.partial(earlier_kernel, count, last),
        out_shape=out_shape,
        in_specs=[pl.BlockSpec(memory_space=pltpu.SMEM), vmem] + [hbm] * count + [vmem] * 3,
        out_specs=out_specs,
        scratch_shapes=scratch,
        input_output_aliases=aliases,
        compiler_params=pltpu.CompilerParams(vmem_limit_bytes=VMEM_LIMIT),
        name="earlier_part_last" if last else "earlier_part",
    )(facts, qt, *shards, *state)


def send(x, by, which=None):
    length = lax.axis_size("ctx")
    pairs = [(i, i + by) for i in range(length - by) if which is None or i % 2 == which]
    return lax.ppermute(x, "ctx", pairs)


def swap(x):
    return lax.ppermute(x, "ctx", [(i, i ^ 1) for i in range(lax.axis_size("ctx"))])


def on_device(queries, key_states, value_states, doc_ids):
    size = key_states.shape[2]
    heads = queries.shape[2] // size
    own = pack(key_states[0], value_states[0], doc_ids)
    four = send(own, 4)
    two = send(own, 2)
    one = send(own, 1, 0)
    qt, *state, facts = own_part(queries[0], own, doc_ids, heads, size)
    four, facts = lax.optimization_barrier((four, facts))
    six = send(four, 2)
    seven = send(four, 3, 1)
    swapped_four = swap(four)
    swapped_two = swap(two)
    early = [one, four, swapped_four, two, swapped_two]
    state = earlier_part(facts, qt, early, state, False)
    six, state = lax.optimization_barrier((six, state))
    swapped_six = swap(six)
    out = earlier_part(facts, qt, [six, seven, swapped_six], state, True)
    return out[None]


def solution(mesh):
    in_specs = (P("dp", "ctx", None), P("dp", "ctx", None), P("dp", "ctx", None), P("dp", "ctx"))
    out_specs = P("dp", "ctx", None)
    return jax.shard_map(
        on_device, mesh=mesh, in_specs=in_specs, out_specs=out_specs, check_vma=False
    )
```

```python
import functools
import math

import jax
import jax.numpy as jnp
from jax import lax
from jax.experimental import pallas as pl
from jax.experimental.pallas import tpu as pltpu
from jax.sharding import PartitionSpec as P


ROWS = 256
META = 16
NEG = -1e30
KEYS = 256
AHEAD = 6
OWN_GROUP = 8
KEY_LIMIT = 4.0
CALM = 100.0
VMEM_LIMIT = 24 << 20


def pack_kernel(*refs):
    sources, (q_ref, out_ref), (k_ref, v_ref, docs_ref, sems) = refs[:4], refs[4:6], refs[6:]
    fetches = [
        pltpu.make_async_copy(source, target, sems.at[i])
        for i, (source, target) in enumerate(zip(sources, (q_ref, k_ref, v_ref, docs_ref)))
    ]
    for fetch in fetches[1:] + fetches[:1]:
        fetch.start()
    for fetch in fetches[1:]:
        fetch.wait()
    tokens, size = k_ref.shape
    out_ref[:tokens, :size] = k_ref[...]
    for start in range(0, tokens, size):
        block = v_ref[start : start + size, :].astype(jnp.float32)
        out_ref[start : start + size, size:] = block.T.astype(jnp.bfloat16)
    width = 2 * size
    ids = (docs_ref[...] + 1).astype(jnp.float32)
    lines = [ids[:, i : i + width] for i in range(0, tokens, width)]
    lines.append(jnp.zeros((META - len(lines), width), jnp.float32))
    out_ref[tokens:, :] = jnp.concatenate(lines, axis=0).astype(jnp.bfloat16)
    fetches[0].wait()


def pack(q, k, v, docs):
    tokens, size = k.shape
    vmem = pl.BlockSpec(memory_space=pltpu.VMEM)
    arrays = [pltpu.with_memory_space_constraint(x, pltpu.HBM) for x in (q, k, v, docs)]
    return pl.pallas_call(
        pack_kernel,
        out_shape=(
            pltpu.VMEM(q.shape, q.dtype),
            pltpu.VMEM((tokens + META, 2 * size), jnp.bfloat16),
        ),
        in_specs=[pl.BlockSpec(memory_space=pltpu.HBM)] * 4,
        out_specs=(vmem, vmem),
        scratch_shapes=[
            pltpu.VMEM(k.shape, k.dtype),
            pltpu.VMEM(v.shape, v.dtype),
            pltpu.VMEM(docs.shape, docs.dtype),
            pltpu.SemaphoreType.DMA((4,)),
        ],
        compiler_params=pltpu.CompilerParams(vmem_limit_bytes=VMEM_LIMIT),
        name="pack",
    )(*arrays)


def keys_twice(kv, start, count, size):
    k = kv[pl.ds(start, count), :size]
    return jnp.concatenate([k, k], axis=1)


def values_across(kv, start, count, size):
    blocks = [kv[pl.ds(start + i, size), size : 2 * size] for i in range(0, count, size)]
    return jnp.concatenate(blocks, axis=1)


def scores_of(keys, q):
    return lax.dot_general(
        keys, q, (((1,), (0,)), ((), ())), preferred_element_type=jnp.float32
    )


def folded(x, op):
    count, width = x.shape
    return op(x.reshape(count // 8, 8, width), axis=0)


def weigh(s, m, l_ref, acc_ref, at, values):
    count, width = s.shape
    p = jnp.exp2(s.reshape(count // 8, 8, width) - m)
    l_ref[at] += jnp.sum(p, axis=0)
    acc_ref[at] += jnp.dot(
        values, p.reshape(count, width).astype(jnp.bfloat16), preferred_element_type=jnp.float32
    )


def weigh_anew(s, m_ref, l_ref, acc_ref, at, values):
    old = m_ref[at]
    top = jnp.max(jnp.maximum(folded(s, jnp.max), old), axis=0, keepdims=True)
    fade = jnp.exp2(old - top)
    m_ref[at] = jnp.broadcast_to(top, old.shape)
    l_ref[at] *= fade
    acc_ref[at] *= fade[:1]
    weigh(s, m_ref[at], l_ref, acc_ref, at, values)


def pipelined(units):
    ahead = [scores() for scores, _ in units[:AHEAD]]
    for i, (_, rest) in enumerate(units):
        if i + AHEAD < len(units):
            ahead.append(units[i + AHEAD][0]())
        rest(ahead.pop(0))


def own_kernel(
    q_ref, own_ref, qt_ref, m_ref, l_ref, acc_ref, facts_ref, bias_ref, kt_ref
):
    tokens = q_ref.shape[0]
    heads, size = acc_ref.shape[0], acc_ref.shape[1]
    scale = size**-0.5 * math.log2(math.e)
    lines = own_ref[tokens:, :].astype(jnp.float32)
    ids = jnp.concatenate([lines[i : i + 1] for i in range(tokens // (2 * size))], axis=1)
    ids_down = jnp.broadcast_to(ids, (size, tokens)).T
    ids_down = jnp.concatenate([ids_down] * (ROWS // size), axis=1)
    for row in range(0, tokens, ROWS):
        count = row + ROWS
        key = lax.broadcasted_iota(jnp.int32, (count, ROWS), 0)
        query = lax.broadcasted_iota(jnp.int32, (count, ROWS), 1) + row
        allowed = (ids_down[:count] == ids[:, row : row + ROWS]) & (key <= query)
        bias_ref[:count, row : row + ROWS] = jnp.where(allowed, 0.0, NEG)
    first = jnp.min(ids)
    facts_ref[0, 1] = first.astype(jnp.int32)
    facts_ref[0, 2] = jnp.sum(jnp.where(ids == first, 1.0, 0.0)).astype(jnp.int32)
    l_ref[...] = jnp.zeros_like(l_ref)
    acc_ref[...] = jnp.zeros_like(acc_ref)
    kt_ref[...] = own_ref[:tokens, :size].T.astype(jnp.float32)

    def prepare(h, gap):
        col = pl.multiple_of(h * size, size)
        scaled = q_ref[:, pl.ds(col, size)].T.astype(jnp.float32) * scale
        high = scaled.astype(jnp.bfloat16)
        low = (scaled - high.astype(jnp.float32)).astype(jnp.bfloat16)
        qt_ref[h, :size, :] = high
        qt_ref[h, size:, :] = low
        own = jnp.sum(scaled * kt_ref[...], axis=0, keepdims=True)
        most = KEY_LIMIT * jnp.sum(jnp.abs(scaled), axis=0, keepdims=True)
        m_ref[h] = jnp.broadcast_to(own, (8, tokens))
        return jnp.maximum(gap, most - own)

    gap = jnp.zeros((1, tokens), jnp.float32)
    for h in range(heads):
        gap = prepare(h, gap)
    calm = jnp.max(gap) <= CALM
    facts_ref[0, 0] = calm.astype(jnp.int32)

    def units(h):
        made = []
        for row in range(0, tokens, ROWS):
            count = row + ROWS
            cols = slice(row, row + ROWS)

            def scores(count=count, cols=cols):
                s = scores_of(keys_twice(own_ref, 0, count, size), qt_ref[h, :, cols])
                return s + bias_ref[:count, cols]

            def rest(s, count=count, cols=cols):
                at, values = (h, slice(None), cols), values_across(own_ref, 0, count, size)
                weigh(s, m_ref[at], l_ref, acc_ref, at, values)

            def rest_anew(s, count=count, cols=cols):
                at, values = (h, slice(None), cols), values_across(own_ref, 0, count, size)
                weigh_anew(s, m_ref, l_ref, acc_ref, at, values)

            made.append((scores, rest, rest_anew))
        return made

    @pl.when(calm)
    def _():
        def body(i, carry):
            group = [u for g in range(OWN_GROUP) for u in units(OWN_GROUP * i + g)]
            pipelined([(scores, rest) for scores, rest, _ in group])
            return carry

        lax.fori_loop(0, heads // OWN_GROUP, body, 0)

    @pl.when(jnp.logical_not(calm))
    def _():
        def body(h, carry):
            pipelined([(scores, rest) for scores, _, rest in units(h)])
            return carry

        lax.fori_loop(0, heads, body, 0)


def own_part(q, own, heads, size):
    tokens = q.shape[0]
    vmem = pl.BlockSpec(memory_space=pltpu.VMEM)
    return pl.pallas_call(
        own_kernel,
        out_shape=(
            jax.ShapeDtypeStruct((heads, 2 * size, tokens), jnp.bfloat16),
            jax.ShapeDtypeStruct((heads, 8, tokens), jnp.float32),
            jax.ShapeDtypeStruct((heads, 8, tokens), jnp.float32),
            jax.ShapeDtypeStruct((heads, size, tokens), jnp.float32),
            jax.ShapeDtypeStruct((1, 3), jnp.int32),
        ),
        in_specs=[vmem, vmem],
        out_specs=(vmem, vmem, vmem, vmem, pl.BlockSpec(memory_space=pltpu.SMEM)),
        scratch_shapes=[
            pltpu.VMEM((tokens, tokens), jnp.float32),
            pltpu.VMEM((size, tokens), jnp.float32),
        ],
        compiler_params=pltpu.CompilerParams(vmem_limit_bytes=VMEM_LIMIT),
        name="own_part",
    )(q, own)


def earlier_kernel(count, last, *refs):
    facts_ref, qt_ref = refs[:2]
    sources = refs[2 : 2 + count]
    m_in, l_in, acc_in = refs[2 + count : 5 + count]
    rest = refs[5 + count :]
    if last:
        out_hbm, m_ref, l_ref, acc_ref = rest[0], m_in, l_in, acc_in
        out_ref, out_sems = rest[-2:]
        rest = rest[1:-2]
    else:
        m_ref, l_ref, acc_ref = rest[:3]
        rest = rest[3:]
    kv_ref, bias_ref, valid_ref = rest
    heads, size, tokens = acc_in.shape
    calm = facts_ref[0, 0] == 1
    first = facts_ref[0, 1].astype(jnp.float32)
    rows = facts_ref[0, 2]

    for j in range(count):
        kv_ref[j] = sources[j][...]
    found = [
        jnp.sum(jnp.where(sources[j][tokens:, :].astype(jnp.float32) == first, 1.0, 0.0))
        for j in range(count)
    ]
    for j in range(count):
        valid_ref[j] = found[j].astype(jnp.int32)

    def unit(kv, h, row, start, keys, bias=None, anew=False):
        at = (h, slice(None), pl.ds(row, ROWS))

        def scores():
            s = scores_of(keys_twice(kv, start, keys, size), qt_ref[at])
            return s if bias is None else s + bias[pl.ds(start, keys), :]

        def rest(s):
            values = values_across(kv, start, keys, size)
            if anew:
                weigh_anew(s, m_ref, l_ref, acc_ref, at, values)
            else:
                query = lax.broadcasted_iota(jnp.int32, (8, ROWS), 1) + row
                m = jnp.where(query < rows, m_ref[at], -NEG)
                weigh(s, m, l_ref, acc_ref, at, values)

        return scores, rest

    def shard(j, carry):
        kv = kv_ref.at[j]
        valid = valid_ref[j]
        whole = calm & (valid == tokens)
        many = rows > tokens - ROWS

        def full(blocks):
            pipelined([
                unit(kv, h, row, start, KEYS)
                for h in range(heads)
                for row in blocks
                for start in range(0, tokens, KEYS)
            ])

        def blocks_of(work):
            def block(i, carry):
                work(pl.multiple_of(i * ROWS, ROWS))
                return carry

            lax.fori_loop(0, (rows + ROWS - 1) // ROWS, block, 0)

        @pl.when(whole & many)
        def _():
            full(range(0, tokens, ROWS))

        @pl.when(whole & jnp.logical_not(many))
        def _():
            blocks_of(lambda row: full([row]))

        def partly(anew, group):
            key = lax.broadcasted_iota(jnp.int32, (tokens, ROWS), 0)
            missing = jnp.where(key >= tokens - valid, 0.0, NEG)

            def work(row):
                query = lax.broadcasted_iota(jnp.int32, (8, ROWS), 1) + row
                if anew:
                    bias_ref[...] = jnp.where((query < rows)[:1], missing, NEG)
                else:
                    bias_ref[...] = missing

                def half(i, carry):
                    start = pl.multiple_of(i * ROWS, ROWS)

                    def some(g, carry):
                        pipelined([
                            unit(kv, group * g + h, row, start, ROWS, bias_ref, anew)
                            for h in range(group)
                        ])
                        return carry

                    if group == heads:
                        some(0, 0)
                    else:
                        lax.fori_loop(0, heads // group, some, 0)
                    return carry

                lax.fori_loop((tokens - valid) // ROWS, tokens // ROWS, half, 0)

            blocks_of(work)

        @pl.when((valid > 0) & calm & jnp.logical_not(whole))
        def _():
            partly(False, heads)

        @pl.when((valid > 0) & jnp.logical_not(calm))
        def _():
            partly(True, 1)

        return carry

    lax.fori_loop(0, count, shard, 0)

    if last:
        copies = []
        for h in range(heads):
            total = jnp.sum(l_ref[h], axis=0, keepdims=True)
            done = (acc_ref[h] * (1.0 / total)).astype(jnp.bfloat16)
            cols = slice(h * size, (h + 1) * size)
            out_ref[:, cols] = done.T
            copies.append(
                pltpu.make_async_copy(out_ref.at[:, cols], out_hbm.at[:, cols], out_sems.at[h])
            )
            copies[-1].start()
        for copy in copies:
            copy.wait()


def earlier_part(facts, qt, shards, state, last):
    heads, double, tokens = qt.shape
    size = double // 2
    count = len(shards)
    vmem = pl.BlockSpec(memory_space=pltpu.VMEM)
    hbm = pl.BlockSpec(memory_space=pltpu.HBM)
    scratch = [
        pltpu.VMEM((count,) + shards[0].shape, jnp.bfloat16),
        pltpu.VMEM((tokens, ROWS), jnp.float32),
        pltpu.SMEM((count,), jnp.int32),
    ]
    if last:
        out_shape = jax.ShapeDtypeStruct((tokens, heads * size), jnp.bfloat16)
        out_specs = hbm
        aliases = {}
        scratch += [pltpu.VMEM(out_shape.shape, jnp.bfloat16), pltpu.SemaphoreType.DMA((heads,))]
    else:
        out_shape = tuple(jax.ShapeDtypeStruct(s.shape, s.dtype) for s in state)
        out_specs = (vmem,) * 3
        aliases = {2 + count + i: i for i in range(3)}
    return pl.pallas_call(
        functools.partial(earlier_kernel, count, last),
        out_shape=out_shape,
        in_specs=[pl.BlockSpec(memory_space=pltpu.SMEM)] + [vmem] * (count + 4),
        out_specs=out_specs,
        scratch_shapes=scratch,
        input_output_aliases=aliases,
        compiler_params=pltpu.CompilerParams(vmem_limit_bytes=VMEM_LIMIT),
        name="earlier_part_last" if last else "earlier_part",
    )(facts, qt, *shards, *state)


def send(x, by, which=None):
    length = lax.axis_size("ctx")
    pairs = [(i, i + by) for i in range(length - by) if which is None or i % 2 == which]
    return lax.ppermute(x, "ctx", pairs)


def swap(x):
    return lax.ppermute(x, "ctx", [(i, i ^ 1) for i in range(lax.axis_size("ctx"))])


def on_device(queries, key_states, value_states, doc_ids):
    size = key_states.shape[2]
    heads = queries.shape[2] // size
    q, own = pack(queries[0], key_states[0], value_states[0], doc_ids)
    four = send(own, 4)
    two = send(own, 2)
    one = send(own, 1, 0)
    qt, *state, facts = own_part(q, own, heads, size)
    four, facts = lax.optimization_barrier((four, facts))
    six = send(four, 2)
    seven = send(four, 3, 1)
    swapped_four = swap(four)
    swapped_two = swap(two)
    state = earlier_part(facts, qt, [one, four, swapped_four, two], state, False)
    six, swapped_two, state = lax.optimization_barrier((six, swapped_two, state))
    swapped_six = swap(six)
    state = earlier_part(facts, qt, [swapped_two, seven], state, False)
    out = earlier_part(facts, qt, [six, swapped_six], state, True)
    return out[None]


def solution(mesh):
    in_specs = (P("dp", "ctx", None), P("dp", "ctx", None), P("dp", "ctx", None), P("dp", "ctx"))
    out_specs = P("dp", "ctx", None)
    return jax.shard_map(
        on_device, mesh=mesh, in_specs=in_specs, out_specs=out_specs, check_vma=False
    )
```
